32 devices in a mesh: gz: 32 (over z, y, x, core), vert: 1.
Axes of the slice: x: 2, y: 2, z: 4, core: 2. Of those that a mesh axis runs over, the one named last changes fastest.
Arguments:
- volume: float32 [256, 128, 1024], P('gz'), may hold values from -6 to 6
- angle_index: int32 [4], P('vert'), may hold values from 0 to 511
- detector_rows: int32 [128], replicated, may hold values from 0 to 127, each once
- measured: float32 [4, 128, 1024], P('vert', 'gz'), may hold values from -96 to 96
Outputs:
- residual: float32 [4, 128, 1024], P('vert', 'gz')
- gradient: float32 [256, 128, 1024], P('gz', 'vert')
The draws below stay inside these ranges and needn't reach their ends.
All inputs are finite; a program needn't handle non-finite values.
Results may differ from the reference program's by a relative error of at most 0.0003.
Values sent between devices are 32-bit elements; how exact they have to be, the bound alone decides.
A program may use at most 64 MiB of HBM per device.

```python
import jax
import jax.numpy as jnp
from jax import lax

X = 1024
ANGLES = 512
NZ = 256
Y = 128
VIEWS = 4


def touch_ends(result, own_key, least, top_value):
    longest = result.shape.index(max(result.shape))
    spots = []
    for shift in (0, 1):
        where = [jax.random.randint(jax.random.fold_in(own_key, axis), (), 0, length) for axis, length in enumerate(result.shape)]
        where[longest] = (where[longest] + shift) % result.shape[longest]
        spots.append(tuple(where))
    return result.at[spots[0]].set(least).at[spots[1]].set(top_value)


def block_levels(rng, extent, pieces, least, high):
    loudness, own = 1.0, jax.random.fold_in(rng, 6)
    for axis_at, shards_of in pieces:
        heights = jnp.exp(jax.random.uniform(jax.random.fold_in(own, axis_at), (shards_of,), jnp.float32, least / len(pieces), high / len(pieces)))
        loudness = loudness * jnp.repeat(heights, extent[axis_at] // shards_of).reshape([-1 if axis == axis_at else 1 for axis in range(len(extent))])
    return loudness


def noise(key, dims, scale, reach, shards=(), kind=jnp.bfloat16):
    result = jax.random.normal(key, dims, jnp.float32) * scale
    if len(shards) > 0:
        result = block_levels(key, dims, shards, -0.22, 0.18) * result
    return jnp.clip(result, min=-reach, max=reach).astype(kind)


def setup_inputs(seed: int = 0) -> dict:
    streams_of = jax.random.split(jax.random.key(seed), 5)
    volume = noise(streams_of[0], (NZ, Y, X), 1.0, 6.0, ((0, 32),), jnp.float32)
    angle_index = touch_ends(jax.random.randint(streams_of[1], (VIEWS,), 0, ANGLES), jax.random.fold_in(streams_of[1], 1), 0, ANGLES - 1).astype(jnp.int32)
    detector_rows = jax.random.permutation(streams_of[2], Y).astype(jnp.int32)
    measured = noise(streams_of[3], (VIEWS, Y, X), 16.0, 96.0, ((1, 32),), jnp.float32)
    return {"volume": volume, "angle_index": angle_index, "detector_rows": detector_rows, "measured": measured}


def shifts(depth_pos, angle_value):
    slope_num = 2 * angle_value - ANGLES
    product = depth_pos * slope_num
    shift_whole = jnp.floor_divide(product, ANGLES)
    shift_part = (product - shift_whole * ANGLES).astype(jnp.float32) / ANGLES
    slope_value = slope_num.astype(jnp.float32) / ANGLES
    weight = jnp.sqrt(1.0 + slope_value * slope_value)
    return (shift_whole.astype(jnp.int32), shift_part, weight)

def reference(volume, angle_index, detector_rows, measured):
    margin = NZ // 2 + 2
    padded = jnp.pad(volume, ((0, 0), (0, 0), (margin, margin)))
    depth_pos = jnp.arange(NZ, dtype=jnp.int32) - NZ // 2

    def project(angle_value):
        shift_whole, shift_part, weight = shifts(depth_pos, angle_value)

        def shifted(plane, offset, fraction):
            window = lax.dynamic_slice_in_dim(plane, offset, X + 1, 1)
            return (1.0 - fraction) * window[:, :-1] + fraction * window[:, 1:]
        contrib = jax.vmap(shifted)(padded, margin + shift_whole, shift_part)
        return weight * lax.optimization_barrier(jnp.sum(contrib, axis=0))
    projection = lax.map(project, angle_index)
    det_order = jnp.take(projection, detector_rows, axis=1)
    residual = (det_order - measured) * NZ ** (-0.5)
    back = jnp.zeros_like(residual).at[:, detector_rows, :].set(residual)
    back_pad = jnp.pad(back, ((0, 0), (0, 0), (margin, margin)))

    def add_view(running, view_item):
        plane, angle_value = view_item
        shift_whole, shift_part, weight = shifts(depth_pos, angle_value)

        def shifted(offset, fraction):
            window = lax.dynamic_slice_in_dim(plane, offset, X + 1, 1)
            return (1.0 - fraction) * window[:, 1:] + fraction * window[:, :-1]
        contrib = jax.vmap(shifted)(margin - shift_whole - 1, shift_part)
        return (running + weight * contrib, None)
    start_sum = jnp.zeros((NZ, Y, X), jnp.float32)
    summed, _ = lax.scan(add_view, start_sum, (back_pad, angle_index))
    gradient = summed * VIEWS ** (-0.5)
    return (residual, gradient)
```

```python
import functools

import jax
import jax.numpy as jnp
from jax import lax
from jax.experimental import pallas as pl
from jax.experimental.pallas import tpu as pltpu
from jax.sharding import PartitionSpec as P

ANGLES = 512
LANES = 128
SUBLANES = 8
COLUMN_PARTS = 2
MESH = pl.DeviceIdType.MESH


def layer_steps(angle, base, layers):
    slope_num = 2 * angle - ANGLES
    rising = slope_num >= 0
    bits = ANGLES.bit_length() - 1
    steps = []
    for i in range(layers):
        layer = jnp.where(rising, i, layers - 1 - i)
        product = (base + layer) * slope_num
        whole = lax.shift_right_arithmetic(product, jnp.int32(bits))
        fraction = (product - whole * ANGLES).astype(jnp.float32) * (1.0 / ANGLES)
        steps.append((layer, whole, fraction))
    return steps


def one_hot_dot(one_hot, values):
    high = values.astype(jnp.bfloat16)
    low = (values - high.astype(jnp.float32)).astype(jnp.bfloat16)
    dot = functools.partial(jnp.dot, preferred_element_type=jnp.float32)
    return dot(one_hot, high) + dot(one_hot, low)


def project_kernel(base_ref, angle_ref, weight_ref, target_ref, vol_ref, out_ref, xs, dxs, partial):
    layers, block_rows, columns = vol_ref.shape
    views, row_count, _ = partial.shape
    width = xs.shape[2]
    step = pl.program_id(0)
    base = base_ref[0]

    def row_group(group, carry):
        rows = pl.ds(pl.multiple_of(group * SUBLANES, SUBLANES), SUBLANES)
        pad = jnp.zeros((SUBLANES, width - columns), jnp.float32)
        for layer in range(layers):
            plane = jnp.concatenate([vol_ref[layer, rows, :], pad], axis=1)
            xs[layer] = plane
            dxs[layer] = pltpu.roll(plane, width - 1, 1) - plane
        for view in range(views):
            steps = layer_steps(angle_ref[view], base, layers)
            total = None
            for i in reversed(range(layers)):
                layer, whole, fraction = steps[i]
                lerp = xs[layer] + fraction * dxs[layer]
                if total is None:
                    total = lerp
                else:
                    moved = steps[i + 1][1] - whole
                    total = lerp + jnp.where(moved == 1, pltpu.roll(total, width - 1, 1), total)
            first = steps[0][1]
            shift = jnp.where(first > 0, width - first, -first)
            total = pltpu.roll(total, shift, 1)[:, :columns] * weight_ref[view]
            out_rows = pl.ds(pl.multiple_of(step * block_rows + group * SUBLANES, SUBLANES), SUBLANES)
            partial[view, out_rows, :] = total
        return carry

    lax.fori_loop(0, block_rows // SUBLANES, row_group, 0)

    @pl.when(step == pl.num_programs(0) - 1)
    def _():
        groups = target_ref.shape[0]
        each = views // groups
        parts = out_ref.shape[0] // groups
        part_columns = columns // parts
        for group in range(groups):
            count = target_ref.shape[1]
            source = lax.broadcasted_iota(jnp.int32, (count, each * row_count), 1)
            one_hot = (target_ref[group] == source).astype(jnp.float32).astype(jnp.bfloat16)
            for part in range(parts):
                values = partial[
                    group * each : (group + 1) * each, :, part * part_columns : (part + 1) * part_columns
                ].reshape(each * row_count, part_columns)
                moved = one_hot_dot(one_hot, values)
                out_ref[group * parts + part] = moved.reshape(out_ref.shape[1:])


def backproject_kernel(base_ref, angle_ref, weight_ref, target_ref, full_ref, out_ref, back):
    layers, block_rows, columns = out_ref.shape
    views, row_count, width = back.shape
    step = pl.program_id(0)
    base = base_ref[0]

    @pl.when(step == 0)
    def _():
        groups = target_ref.shape[0]
        each = views // groups
        parts = full_ref.shape[0] // groups
        part_columns = columns // parts
        for view in range(views):
            back[view, :, columns:] = jnp.zeros((row_count, width - columns), jnp.float32)
        for group in range(groups):
            count = target_ref.shape[2]
            source = lax.broadcasted_iota(jnp.int32, (each * row_count, count), 0)
            one_hot = (target_ref[group] == source).astype(jnp.float32).astype(jnp.bfloat16)
            for part in range(parts):
                values = full_ref[group * parts + part].reshape(count, part_columns)
                moved = one_hot_dot(one_hot, values).reshape(each, row_count, part_columns)
                for i in range(each):
                    view = group * each + i
                    back[view, :, part * part_columns : (part + 1) * part_columns] = (
                        moved[i] * weight_ref[view]
                    )

    def row_group(group, carry):
        rows = pl.ds(pl.multiple_of(group * SUBLANES, SUBLANES), SUBLANES)
        back_rows = pl.ds(pl.multiple_of(step * block_rows + group * SUBLANES, SUBLANES), SUBLANES)
        for view in range(views):
            steps = layer_steps(angle_ref[view], base, layers)
            first = steps[0][1]
            shift = jnp.where(first < 0, width + first, first)
            current = pltpu.roll(back[view, back_rows, :], shift, 1)
            for i in range(layers):
                layer, whole, fraction = steps[i]
                after = pltpu.roll(current, 1, 1)
                contrib = (current + fraction * (after - current))[:, :columns]
                if view == 0:
                    out_ref[layer, rows, :] = contrib
                else:
                    out_ref[layer, rows, :] += contrib
                if i + 1 < layers:
                    current = jnp.where(steps[i + 1][1] - whole == 1, after, current)
        return carry

    lax.fori_loop(0, block_rows // SUBLANES, row_group, 0)


def exchange_kernel(n, orders, scale, in_ref, meas_ref, res_ref, full_ref,
                    got0, got1, got2, got3, put1, put2, put3, send_sem, recv_sem):
    me = lax.axis_index("gz")
    high_count = n // 8
    core, bit1, bit2, high = me % 2, (me // 2) % 2, (me // 4) % 2, me // 8
    other_core = me + 1 - 2 * core
    other1, other2 = me + 2 - 4 * bit1, me + 4 - 8 * bit2
    others = [me + 8 * (lax.rem(high + j, high_count) - high) for j in range(1, high_count)]
    count = in_ref.shape[0]
    part_columns = in_ref.shape[-1]
    per_group = count // meas_ref.shape[0]

    barrier = pltpu.get_barrier_semaphore()
    for peer in [other_core, other1, other2] + others:
        pl.semaphore_signal(barrier, inc=1, device_id={"gz": peer}, device_id_type=MESH)
    pl.semaphore_wait(barrier, 3 + len(others))

    started = {}

    def start(part, stage, source, target, peer):
        copy = pltpu.make_async_remote_copy(
            src_ref=source, dst_ref=target,
            send_sem=send_sem.at[part, stage], recv_sem=recv_sem.at[part, stage],
            device_id={"gz": peer}, device_id_type=MESH,
        )
        copy.start()
        started[part, stage] = copy

    def arrived(part, stage):
        started[part, stage].wait_recv()

    def ends(part):
        if orders[part] == 0:
            return bit1, bit2, other1, other2
        return bit2, bit1, other2, other1

    parts = range(count)
    for part in parts:
        start(part, 0, in_ref.at[part, 1 - core], got0.at[part], other_core)
    for part in parts:
        a, b, peer_a, peer_b = ends(part)
        arrived(part, 0)
        put1[part] = in_ref[part, core, 1 - a] + got0[part, 1 - a]
        start(part, 1, put1.at[part], got1.at[part], peer_a)
    for part in parts:
        a, b, peer_a, peer_b = ends(part)
        arrived(part, 1)
        put2[part] = in_ref[part, core, a, 1 - b] + got0[part, a, 1 - b] + got1[part, 1 - b]
        start(part, 2, put2.at[part], got2.at[part], peer_b)
    for part in parts:
        a, b, peer_a, peer_b = ends(part)
        arrived(part, 2)
        put3[part] = in_ref[part, core, a, b] + got0[part, a, b] + got1[part, b] + got2[part]
        for j, peer in enumerate(others):
            start(part, 3 + j, put3.at[part, lax.rem(high + j + 1, high_count)], got3.at[part, j], peer)
    gather = 3 + len(others)
    for part in parts:
        a, b, peer_a, peer_b = ends(part)
        total = put3[part, high]
        for j in range(len(others)):
            arrived(part, 3 + j)
            total = total + got3[part, j]
        group, column = part // per_group, (part % per_group) * part_columns
        residual = (total - meas_ref[group, :, column : column + part_columns]) * scale
        res_ref[group, :, column : column + part_columns] = residual
        full_ref[part, core, a, b, high] = residual
        mine = full_ref.at[part, core, a, b, high]
        for j, peer in enumerate(others):
            start(part, gather + j, mine, mine, peer)
    last = gather + len(others)
    for part in parts:
        a, b, peer_a, peer_b = ends(part)
        for j in range(len(others)):
            arrived(part, gather + j)
        mine = full_ref.at[part, core, a, b]
        start(part, last, mine, mine, peer_b)
    for part in parts:
        a, b, peer_a, peer_b = ends(part)
        arrived(part, last)
        mine = full_ref.at[part, core, a]
        start(part, last + 1, mine, mine, peer_a)
    for part in parts:
        arrived(part, last + 1)
        mine = full_ref.at[part, core]
        start(part, last + 2, mine, mine, other_core)
    for part in parts:
        arrived(part, last + 2)
    for copy in started.values():
        copy.wait_send()


def per_device(volume, angle_index, detector_rows, measured):
    layers, row_count, columns = volume.shape
    views = angle_index.shape[0]
    n = lax.axis_size("gz")
    total_depth = layers * n
    own_rows = row_count // n
    each = SUBLANES // own_rows
    groups = views // each
    high_count = n // 8
    margin = -(-(total_depth // 2) // LANES) * LANES
    width = columns + 2 * margin
    part_columns = columns // COLUMN_PARTS
    count = groups * COLUMN_PARTS
    orders = tuple((part // COLUMN_PARTS) % 2 for part in range(count))
    block_rows = 32
    res_scale = total_depth ** (-0.5)
    view_scale = (views * lax.axis_size("vert")) ** (-0.5)

    base = (lax.axis_index("gz") * layers - total_depth // 2).astype(jnp.int32).reshape(1)
    slope = (2 * angle_index - ANGLES).astype(jnp.float32) / ANGLES
    weight = jnp.sqrt(1.0 + slope * slope)

    by_bits = detector_rows.reshape(high_count, 2, 2, 2, own_rows)
    targets = []
    for group in range(groups):
        order = (3, 2, 1, 0, 4) if group % 2 == 0 else (3, 1, 2, 0, 4)
        placed = jnp.transpose(by_bits, order).reshape(n, 1, own_rows)
        placed = placed + (jnp.arange(each, dtype=jnp.int32) * row_count)[None, :, None]
        targets.append(placed.reshape(-1))
    target = jnp.stack(targets)

    smem = pl.BlockSpec(memory_space=pltpu.SMEM)
    vmem = pl.BlockSpec(memory_space=pltpu.VMEM)
    full_shape = (count, 2, 2, 2, high_count, SUBLANES, part_columns)
    half = (SUBLANES, part_columns)
    whole = pl.BlockSpec(full_shape, lambda i: (0,) * len(full_shape))
    partials = pl.pallas_call(
        project_kernel,
        grid=(row_count // block_rows,),
        out_shape=jax.ShapeDtypeStruct(full_shape, jnp.float32),
        in_specs=[
            smem, smem, smem,
            pl.BlockSpec((groups, target.shape[1], 1), lambda i: (0, 0, 0)),
            pl.BlockSpec((layers, block_rows, columns), lambda i: (0, i, 0)),
        ],
        out_specs=whole,
        scratch_shapes=[
            pltpu.VMEM((layers, SUBLANES, width), jnp.float32),
            pltpu.VMEM((layers, SUBLANES, width), jnp.float32),
            pltpu.VMEM((views, row_count, columns), jnp.float32),
        ],
        name="project",
    )(base, angle_index, weight, target[:, :, None], volume)

    others = high_count - 1
    stages = 6 + 2 * others
    residual, full = pl.pallas_call(
        functools.partial(exchange_kernel, n, orders, res_scale),
        out_shape=(
            jax.ShapeDtypeStruct((groups, SUBLANES, columns), jnp.float32),
            jax.ShapeDtypeStruct(full_shape, jnp.float32),
        ),
        in_specs=[vmem, vmem],
        out_specs=(vmem, vmem),
        scratch_shapes=[
            pltpu.VMEM((count, 2, 2, high_count) + half, jnp.float32),
            pltpu.VMEM((count, 2, high_count) + half, jnp.float32),
            pltpu.VMEM((count, high_count) + half, jnp.float32),
            pltpu.VMEM((count, others) + half, jnp.float32),
            pltpu.VMEM((count, 2, high_count) + half, jnp.float32),
            pltpu.VMEM((count, high_count) + half, jnp.float32),
            pltpu.VMEM((count, high_count) + half, jnp.float32),
            pltpu.SemaphoreType.DMA((count, stages)),
            pltpu.SemaphoreType.DMA((count, stages)),
        ],
        compiler_params=pltpu.CompilerParams(collective_id=0, has_side_effects=True),
        name="exchange",
    )(partials, measured.reshape(groups, SUBLANES, columns))

    gradient = pl.pallas_call(
        backproject_kernel,
        grid=(row_count // block_rows,),
        out_shape=jax.ShapeDtypeStruct((layers, row_count, columns), jnp.float32),
        in_specs=[
            smem, smem, smem,
            pl.BlockSpec((groups, 1, target.shape[1]), lambda i: (0, 0, 0)),
            whole,
        ],
        out_specs=pl.BlockSpec((layers, block_rows, columns), lambda i: (0, i, 0)),
        scratch_shapes=[pltpu.VMEM((views, row_count, width), jnp.float32)],
        name="backproject",
    )(base, angle_index, weight * view_scale, target[:, None, :], full)
    gradient = lax.psum_scatter(gradient, "vert", scatter_dimension=1, tiled=True)
    return (residual.reshape(measured.shape), gradient)


def solution(mesh):
    in_specs = (P("gz", None, None), P("vert"), P(), P("vert", "gz", None))
    out_specs = (P("vert", "gz", None), P("gz", "vert", None))
    return jax.shard_map(
        per_device, mesh=mesh, in_specs=in_specs, out_specs=out_specs, check_vma=False
    )
```

```python
import functools

import jax
import jax.numpy as jnp
from jax import lax
from jax.experimental import pallas as pl
from jax.experimental.pallas import tpu as pltpu
from jax.sharding import PartitionSpec as P

ANGLES = 512
LANES = 128
SUBLANES = 8
COLUMN_PARTS = 2
CHUNK = 64
MESH = pl.DeviceIdType.MESH


def log2(value):
    return value.bit_length() - 1


def shift_parts(depth, angle):
    product = depth * (2 * angle - ANGLES)
    whole = lax.shift_right_arithmetic(product, jnp.int32(log2(ANGLES)))
    fraction = (product - whole * ANGLES).astype(jnp.float32) * (1.0 / ANGLES)
    return whole, fraction


def ray_weight(angle):
    slope = (2 * angle - ANGLES).astype(jnp.float32) * (1.0 / ANGLES)
    return jnp.sqrt(jnp.full((1, LANES), 1.0 + slope * slope, jnp.float32))


def row_places(det_ref, n, each, own_rows, order):
    row_count = det_ref.shape[1]
    count = n * each * own_rows
    place = lax.broadcasted_iota(jnp.int32, (count, row_count), 0)
    detector = lax.broadcasted_iota(jnp.int32, (count, row_count), 1)
    row = place & (own_rows - 1)
    view = lax.shift_right_logical(place, log2(own_rows)) & (each - 1)
    slot = lax.shift_right_logical(place, log2(own_rows * each))
    high_count = n // 8
    high = slot & (high_count - 1)
    bits = lax.shift_right_logical(slot, log2(high_count))
    second, first, core = bits & 1, lax.shift_right_logical(bits, 1) & 1, lax.shift_right_logical(bits, 2)
    bit1, bit2 = (first, second) if order == 0 else (second, first)
    owner = high * 8 + bit2 * 4 + bit1 * 2 + core
    from_detector = (owner * own_rows + row) == detector
    volume_row = lax.broadcasted_iota(jnp.int32, (row_count, row_count), 0)
    records = (det_ref[...] == volume_row).astype(jnp.float32).astype(jnp.bfloat16)
    places = []
    for i in range(each):
        pick = (from_detector & (view == i)).astype(jnp.float32).astype(jnp.bfloat16)
        moved = lax.dot_general(pick, records, (((1,), (1,)), ((), ())), preferred_element_type=jnp.float32)
        places.append(moved.astype(jnp.bfloat16))
    return places


def two_terms(values):
    high = values.astype(jnp.bfloat16)
    return high, (values - high.astype(jnp.float32)).astype(jnp.bfloat16)


def place_dot(a, b, dims):
    return lax.dot_general(a, b, (dims, ((), ())), preferred_element_type=jnp.float32)


def project_kernel(n, total_depth, angle_ref, det_ref, vol_ref, out_ref, planes, partial):
    layers, height, _ = planes.shape
    views, columns, row_count = partial.shape
    margin = (height - columns) // 2
    layer = pl.program_id(0)
    base = lax.axis_index("gz") * layers - total_depth // 2

    blank = jnp.zeros((margin, row_count), jnp.float32)
    planes[layer, :margin, :] = blank
    planes[layer, margin + columns :, :] = blank
    for column in range(0, columns, LANES):
        planes[layer, margin + column : margin + column + LANES, :] = vol_ref[0, :, column : column + LANES].T

    @pl.when(layer == layers - 1)
    def _():
        for view in range(views):
            steps = [shift_parts(base + i, angle_ref[view]) for i in range(layers)]
            weight = ray_weight(angle_ref[view])

            def chunk(index, carry):
                at = pl.multiple_of(index * CHUNK, CHUNK)
                total = jnp.zeros((CHUNK, row_count), jnp.float32)
                for i, (whole, fraction) in enumerate(steps):
                    here = planes[i, pl.ds(margin + at + whole, CHUNK), :]
                    following = planes[i, pl.ds(margin + at + whole + 1, CHUNK), :]
                    total = total + ((1.0 - fraction) * here + fraction * following)
                partial[view, pl.ds(at, CHUNK), :] = total * weight
                return carry

            lax.fori_loop(0, columns // CHUNK, chunk, 0)

        own_rows = row_count // n
        each = SUBLANES // own_rows
        groups = views // each
        parts = out_ref.shape[0] // groups
        width = columns // parts
        for part in range(parts):
            places = row_places(det_ref, n, each, own_rows, part % 2)
            for group in range(groups):
                moved = 0.0
                for i in range(each):
                    for term in two_terms(partial[group * each + i, part * width : (part + 1) * width, :]):
                        moved = moved + place_dot(places[i], term, ((1,), (1,)))
                out_ref[group * parts + part] = moved.reshape(out_ref.shape[1:])


def backproject_kernel(n, total_depth, view_scale, angle_ref, det_ref, full_ref, out_ref, back):
    views, height, row_count = back.shape
    _, _, columns = out_ref.shape
    layers = pl.num_programs(0)
    margin = (height - columns) // 2
    layer = pl.program_id(0)
    depth = lax.axis_index("gz") * layers - total_depth // 2 + layer

    @pl.when(layer == 0)
    def _():
        own_rows = row_count // n
        each = SUBLANES // own_rows
        groups = views // each
        parts = full_ref.shape[0] // groups
        width = columns // parts
        blank = jnp.zeros((margin, row_count), jnp.float32)
        for view in range(views):
            back[view, :margin, :] = blank
            back[view, margin + columns :, :] = blank
        for part in range(parts):
            places = row_places(det_ref, n, each, own_rows, part % 2)
            for group in range(groups):
                terms = two_terms(full_ref[group * parts + part].reshape(-1, width).T)
                for i in range(each):
                    view = group * each + i
                    moved = place_dot(terms[0], places[i], ((1,), (0,))) + place_dot(
                        terms[1], places[i], ((1,), (0,))
                    )
                    back[view, margin + part * width : margin + (part + 1) * width, :] = moved * (
                        ray_weight(angle_ref[view]) * view_scale
                    )

    steps = [shift_parts(depth, angle_ref[view]) for view in range(views)]

    def chunk(index, carry):
        at = pl.multiple_of(index * LANES, LANES)
        total = jnp.zeros((LANES, row_count), jnp.float32)
        for view, (whole, fraction) in enumerate(steps):
            here = back[view, pl.ds(margin + at - whole, LANES), :]
            before = back[view, pl.ds(margin + at - whole - 1, LANES), :]
            total = total + ((1.0 - fraction) * here + fraction * before)
        out_ref[0, :, pl.ds(at, LANES)] = total.T
        return carry

    lax.fori_loop(0, columns // LANES, chunk, 0)


def exchange_kernel(n, orders, scale, in_ref, meas_ref, res_ref, full_ref,
                    got0, got1, got2, got3, put1, put2, put3, send_sem, recv_sem):
    me = lax.axis_index("gz")
    high_count = n // 8
    core, bit1, bit2, high = me % 2, (me // 2) % 2, (me // 4) % 2, me // 8
    other_core = me + 1 - 2 * core
    other1, other2 = me + 2 - 4 * bit1, me + 4 - 8 * bit2
    others = [me + 8 * (lax.rem(high + j, high_count) - high) for j in range(1, high_count)]
    count = in_ref.shape[0]
    part_columns = in_ref.shape[-1]
    own_rows = meas_ref.shape[1]
    each = SUBLANES // own_rows
    per_group = count * each // meas_ref.shape[0]

    barrier = pltpu.get_barrier_semaphore()
    for peer in [other_core, other1, other2] + others:
        pl.semaphore_signal(barrier, inc=1, device_id={"gz": peer}, device_id_type=MESH)
    pl.semaphore_wait(barrier, 3 + len(others))

    started = {}

    def start(part, stage, source, target, peer):
        copy = pltpu.make_async_remote_copy(
            src_ref=source, dst_ref=target,
            send_sem=send_sem.at[part, stage], recv_sem=recv_sem.at[part, stage],
            device_id={"gz": peer}, device_id_type=MESH,
        )
        copy.start()
        started[part, stage] = copy

    def arrived(part, stage):
        started[part, stage].wait_recv()

    def ends(part):
        if orders[part] == 0:
            return bit1, bit2, other1, other2
        return bit2, bit1, other2, other1

    parts = range(count)
    for part in parts:
        start(part, 0, in_ref.at[part, 1 - core], got0.at[part], other_core)
    for part in parts:
        a, b, peer_a, peer_b = ends(part)
        arrived(part, 0)
        put1[part] = in_ref[part, core, 1 - a] + got0[part, 1 - a]
        start(part, 1, put1.at[part], got1.at[part], peer_a)
    for part in parts:
        a, b, peer_a, peer_b = ends(part)
        arrived(part, 1)
        put2[part] = in_ref[part, core, a, 1 - b] + got0[part, a, 1 - b] + got1[part, 1 - b]
        start(part, 2, put2.at[part], got2.at[part], peer_b)
    for part in parts:
        a, b, peer_a, peer_b = ends(part)
        arrived(part, 2)
        put3[part] = in_ref[part, core, a, b] + got0[part, a, b] + got1[part, b] + got2[part]
        for j, peer in enumerate(others):
            start(part, 3 + j, put3.at[part, lax.rem(high + j + 1, high_count)], got3.at[part, j], peer)
    gather = 3 + len(others)
    for part in parts:
        a, b, peer_a, peer_b = ends(part)
        total = put3[part, high]
        for j in range(len(others)):
            arrived(part, 3 + j)
            total = total + got3[part, j]
        group, column = part // per_group, (part % per_group) * part_columns
        wanted = [meas_ref[group * each + i, :, column : column + part_columns] for i in range(each)]
        residual = (total - jnp.concatenate(wanted, axis=0)) * scale
        for i in range(each):
            res_ref[group * each + i, :, column : column + part_columns] = residual[
                i * own_rows : (i + 1) * own_rows
            ]
        full_ref[part, core, a, b, high] = residual
        mine = full_ref.at[part, core, a, b, high]
        for j, peer in enumerate(others):
            start(part, gather + j, mine, mine, peer)
    last = gather + len(others)
    for part in parts:
        a, b, peer_a, peer_b = ends(part)
        for j in range(len(others)):
            arrived(part, gather + j)
        mine = full_ref.at[part, core, a, b]
        start(part, last, mine, mine, peer_b)
    for part in parts:
        a, b, peer_a, peer_b = ends(part)
        arrived(part, last)
        mine = full_ref.at[part, core, a]
        start(part, last + 1, mine, mine, peer_a)
    for part in parts:
        arrived(part, last + 1)
        mine = full_ref.at[part, core]
        start(part, last + 2, mine, mine, other_core)
    for part in parts:
        arrived(part, last + 2)
    for copy in started.values():
        copy.wait_send()


def per_device(volume, angle_index, detector_rows, measured):
    layers, row_count, columns = volume.shape
    views = angle_index.shape[0]
    n = lax.axis_size("gz")
    total_depth = layers * n
    own_rows = row_count // n
    each = SUBLANES // own_rows
    groups = views // each
    high_count = n // 8
    height = columns + 2 * (total_depth // 2 + SUBLANES)
    part_columns = columns // COLUMN_PARTS
    count = groups * COLUMN_PARTS
    orders = tuple((part % COLUMN_PARTS) % 2 for part in range(count))
    res_scale = total_depth ** (-0.5)
    view_scale = (views * lax.axis_size("vert")) ** (-0.5)
    detectors = detector_rows.reshape(1, row_count)

    smem = pl.BlockSpec(memory_space=pltpu.SMEM)
    vmem = pl.BlockSpec(memory_space=pltpu.VMEM)
    full_shape = (count, 2, 2, 2, high_count, SUBLANES, part_columns)
    half = (SUBLANES, part_columns)
    whole = pl.BlockSpec(full_shape, lambda i: (0,) * len(full_shape))
    one_row = pl.BlockSpec((1, row_count), lambda i: (0, 0))
    plane = pl.BlockSpec((1, row_count, columns), lambda i: (i, 0, 0))
    partials = pl.pallas_call(
        functools.partial(project_kernel, n, total_depth),
        grid=(layers,),
        out_shape=jax.ShapeDtypeStruct(full_shape, jnp.float32),
        in_specs=[smem, one_row, plane],
        out_specs=whole,
        scratch_shapes=[
            pltpu.VMEM((layers, height, row_count), jnp.float32),
            pltpu.VMEM((views, columns, row_count), jnp.float32),
        ],
        name="project",
    )(angle_index, detectors, volume)

    others = high_count - 1
    stages = 6 + 2 * others
    residual, full = pl.pallas_call(
        functools.partial(exchange_kernel, n, orders, res_scale),
        out_shape=(
            jax.ShapeDtypeStruct(measured.shape, jnp.float32),
            jax.ShapeDtypeStruct(full_shape, jnp.float32),
        ),
        in_specs=[vmem, vmem],
        out_specs=(vmem, vmem),
        scratch_shapes=[
            pltpu.VMEM((count, 2, 2, high_count) + half, jnp.float32),
            pltpu.VMEM((count, 2, high_count) + half, jnp.float32),
            pltpu.VMEM((count, high_count) + half, jnp.float32),
            pltpu.VMEM((count, others) + half, jnp.float32),
            pltpu.VMEM((count, 2, high_count) + half, jnp.float32),
            pltpu.VMEM((count, high_count) + half, jnp.float32),
            pltpu.VMEM((count, high_count) + half, jnp.float32),
            pltpu.SemaphoreType.DMA((count, stages)),
            pltpu.SemaphoreType.DMA((count, stages)),
        ],
        compiler_params=pltpu.CompilerParams(collective_id=0, has_side_effects=True),
        name="exchange",
    )(partials, measured)

    gradient = pl.pallas_call(
        functools.partial(backproject_kernel, n, total_depth, view_scale),
        grid=(layers,),
        out_shape=jax.ShapeDtypeStruct((layers, row_count, columns), jnp.float32),
        in_specs=[smem, one_row, whole],
        out_specs=plane,
        scratch_shapes=[pltpu.VMEM((views, height, row_count), jnp.float32)],
        name="backproject",
    )(angle_index, detectors, full)
    gradient = lax.psum_scatter(gradient, "vert", scatter_dimension=1, tiled=True)
    return (residual, gradient)


def solution(mesh):
    in_specs = (P("gz", None, None), P("vert"), P(), P("vert", "gz", None))
    out_specs = (P("vert", "gz", None), P("gz", "vert", None))
    return jax.shard_map(
        per_device, mesh=mesh, in_specs=in_specs, out_specs=out_specs, check_vma=False
    )
```

```python
import functools

import jax
import jax.numpy as jnp
from jax import lax
from jax.experimental import pallas as pl
from jax.experimental.pallas import tpu as pltpu
from jax.sharding import PartitionSpec as P

ANGLES = 512
LANES = 128
SUBLANES = 8
COLUMN_PARTS = 4
STAGGER = 0.4
VMEM_LIMIT = 36 * 2**20
CHUNK = 64
MESH = pl.DeviceIdType.MESH


def log2(value):
    return value.bit_length() - 1


def shift_parts(depth, angle):
    product = depth * (2 * angle - ANGLES)
    whole = lax.shift_right_arithmetic(product, jnp.int32(log2(ANGLES)))
    fraction = (product - whole * ANGLES).astype(jnp.float32) * (1.0 / ANGLES)
    return whole, fraction


def ray_weight(angle):
    slope = (2 * angle - ANGLES).astype(jnp.float32) * (1.0 / ANGLES)
    return jnp.sqrt(jnp.full((1, LANES), 1.0 + slope * slope, jnp.float32))


def row_places(det_ref, n, each, own_rows, order):
    row_count = det_ref.shape[1]
    count = n * each * own_rows
    place = lax.broadcasted_iota(jnp.int32, (count, row_count), 0)
    detector = lax.broadcasted_iota(jnp.int32, (count, row_count), 1)
    row = place & (own_rows - 1)
    view = lax.shift_right_logical(place, log2(own_rows)) & (each - 1)
    slot = lax.shift_right_logical(place, log2(own_rows * each))
    high_count = n // 8
    high = slot & (high_count - 1)
    bits = lax.shift_right_logical(slot, log2(high_count))
    second, first, core = bits & 1, lax.shift_right_logical(bits, 1) & 1, lax.shift_right_logical(bits, 2)
    bit1, bit2 = (first, second) if order == 0 else (second, first)
    owner = high * 8 + bit2 * 4 + bit1 * 2 + core
    from_detector = (owner * own_rows + row) == detector
    volume_row = lax.broadcasted_iota(jnp.int32, (row_count, row_count), 0)
    records = (det_ref[...] == volume_row).astype(jnp.float32).astype(jnp.bfloat16)
    places = []
    for i in range(each):
        pick = (from_detector & (view == i)).astype(jnp.float32).astype(jnp.bfloat16)
        moved = lax.dot_general(pick, records, (((1,), (1,)), ((), ())), preferred_element_type=jnp.float32)
        places.append(moved.astype(jnp.bfloat16))
    return places


def two_terms(values):
    high = values.astype(jnp.bfloat16)
    return high, (values - high.astype(jnp.float32)).astype(jnp.bfloat16)


def place_dot(a, b, dims):
    return lax.dot_general(a, b, (dims, ((), ())), preferred_element_type=jnp.float32)


def forward_kernel(n, orders, total_depth, scale, view_scale, angle_ref, det_ref, meas_ref, vol_ref,
                   res_ref, back_ref, slabs, planes, places, partial, own, full,
                   got0, got1, got2, got3, put1, put2, put3, load_sem, send_sem, recv_sem):
    layers, height, row_count = planes.shape
    views, own_rows, columns = meas_ref.shape
    margin = (height - columns) // 2
    each = SUBLANES // own_rows
    count, width = own.shape[0], own.shape[-1]
    per_group = count * each // views

    me = lax.axis_index("gz")
    high_count = n // 8
    core, bit1, bit2, high = me % 2, (me // 2) % 2, (me // 4) % 2, me // 8
    other_core = me + 1 - 2 * core
    other1, other2 = me + 2 - 4 * bit1, me + 4 - 8 * bit2
    others = [me + 8 * (lax.rem(high + j, high_count) - high) for j in range(1, high_count)]
    base = me * layers - total_depth // 2

    loads = [
        pltpu.make_async_copy(vol_ref.at[layer], slabs.at[layer], load_sem.at[layer]) for layer in range(layers)
    ]
    for load in loads:
        load.start()
    barrier = pltpu.get_barrier_semaphore()
    for peer in [other_core, other1, other2] + others:
        pl.semaphore_signal(barrier, inc=1, device_id={"gz": peer}, device_id_type=MESH)

    blank = jnp.zeros((margin, row_count), jnp.float32)
    for layer in range(layers):
        planes[layer, :margin, :] = blank
        planes[layer, margin + columns :, :] = blank
    for view in range(views):
        back_ref[view, :margin, :] = blank
        back_ref[view, margin + columns :, :] = blank
    for order in range(2):
        for i, place in enumerate(row_places(det_ref, n, each, own_rows, order)):
            places[order, i] = place
    for layer in range(layers):
        loads[layer].wait()

        def turn(index, carry):
            at = pl.multiple_of(index * LANES, LANES)
            planes[layer, pl.ds(pl.multiple_of(margin + at, SUBLANES), LANES), :] = slabs[layer, :, pl.ds(at, LANES)].T
            return carry

        lax.fori_loop(0, columns // LANES, turn, 0, unroll=True)
    pl.semaphore_wait(barrier, 3 + len(others))

    started = {}
    gather = 3 + len(others)
    last = gather + len(others)

    def start(part, stage, source, target, peer):
        copy = pltpu.make_async_remote_copy(
            src_ref=source, dst_ref=target,
            send_sem=send_sem.at[part, stage], recv_sem=recv_sem.at[part, stage],
            device_id={"gz": peer}, device_id_type=MESH,
        )
        copy.start()
        started[part, stage] = copy

    def arrived(part, stage):
        started[part, stage].wait_recv()

    def project(part):
        group, left = part // per_group, (part % per_group) * width
        moved = 0.0
        for i in range(each):
            angle = angle_ref[group * each + i]
            steps = [shift_parts(base + layer, angle) for layer in range(layers)]
            weight = ray_weight(angle)

            def chunk(index, carry):
                at = pl.multiple_of(index * CHUNK, CHUNK)
                total = jnp.zeros((CHUNK, row_count), jnp.float32)
                for layer, (whole, fraction) in enumerate(steps):
                    first = margin + left + at + whole
                    here = planes[layer, pl.ds(first, CHUNK), :]
                    following = planes[layer, pl.ds(first + 1, CHUNK), :]
                    total = total + ((1.0 - fraction) * here + fraction * following)
                partial[i, pl.ds(at, CHUNK), :] = total * weight
                return carry

            lax.fori_loop(0, width // CHUNK, chunk, 0)
            for term in two_terms(partial[i]):
                moved = moved + place_dot(places[orders[part], i], term, ((1,), (1,)))
        own[part] = moved.reshape(own.shape[1:])

    def place(part):
        group, left = part // per_group, (part % per_group) * width
        terms = two_terms(full[part].reshape(-1, width).T)
        for i in range(each):
            view = group * each + i
            matrix = places[orders[part], i]
            moved = place_dot(terms[0], matrix, ((1,), (0,))) + place_dot(terms[1], matrix, ((1,), (0,)))
            back_ref[view, margin + left : margin + left + width, :] = moved * (
                ray_weight(angle_ref[view]) * view_scale
            )

    def event(part, stage):
        if orders[part] == 0:
            a, b, peer_a, peer_b = bit1, bit2, other1, other2
        else:
            a, b, peer_a, peer_b = bit2, bit1, other2, other1
        if stage == 0:
            project(part)
            start(part, 0, own.at[part, 1 - core], got0.at[part], other_core)
        elif stage == 1:
            arrived(part, 0)
            put1[part] = own[part, core, 1 - a] + got0[part, 1 - a]
            start(part, 1, put1.at[part], got1.at[part], peer_a)
        elif stage == 2:
            arrived(part, 1)
            put2[part] = own[part, core, a, 1 - b] + got0[part, a, 1 - b] + got1[part, 1 - b]
            start(part, 2, put2.at[part], got2.at[part], peer_b)
        elif stage == 3:
            arrived(part, 2)
            put3[part] = own[part, core, a, b] + got0[part, a, b] + got1[part, b] + got2[part]
            for j, peer in enumerate(others):
                start(part, 3 + j, put3.at[part, lax.rem(high + j + 1, high_count)], got3.at[part, j], peer)
        elif stage == 4:
            total = put3[part, high]
            for j in range(len(others)):
                arrived(part, 3 + j)
                total = total + got3[part, j]
            group, column = part // per_group, (part % per_group) * width
            wanted = [meas_ref[group * each + i, :, column : column + width] for i in range(each)]
            residual = (total - jnp.concatenate(wanted, axis=0)) * scale
            full[part, core, a, b, high] = residual
            mine = full.at[part, core, a, b, high]
            for j, peer in enumerate(others):
                start(part, gather + j, mine, mine, peer)
            for i in range(each):
                res_ref[group * each + i, :, column : column + width] = residual[i * own_rows : (i + 1) * own_rows]
        elif stage == 5:
            for j in range(len(others)):
                arrived(part, gather + j)
            mine = full.at[part, core, a, b]
            start(part, last, mine, mine, peer_b)
        elif stage == 6:
            arrived(part, last)
            mine = full.at[part, core, a]
            start(part, last + 1, mine, mine, peer_a)
        elif stage == 7:
            arrived(part, last + 1)
            mine = full.at[part, core]
            start(part, last + 2, mine, mine, other_core)
        else:
            arrived(part, last + 2)
            place(part)

    for stage, part in sorted(
        ((stage, part) for stage in range(9) for part in range(count)),
        key=lambda item: (item[0] + STAGGER * item[1], -item[0]),
    ):
        event(part, stage)
    for copy in started.values():
        copy.wait_send()


def backproject_kernel(total_depth, angle_ref, back_ref, out_ref):
    views, height, row_count = back_ref.shape
    columns = out_ref.shape[2]
    layers = pl.num_programs(0)
    margin = (height - columns) // 2
    depth = lax.axis_index("gz") * layers - total_depth // 2 + pl.program_id(0)
    steps = [shift_parts(depth, angle_ref[view]) for view in range(views)]

    def chunk(index, carry):
        at = pl.multiple_of(index * LANES, LANES)
        total = jnp.zeros((LANES, row_count), jnp.float32)
        for view, (whole, fraction) in enumerate(steps):
            here = back_ref[view, pl.ds(margin + at - whole, LANES), :]
            before = back_ref[view, pl.ds(margin + at - whole - 1, LANES), :]
            total = total + ((1.0 - fraction) * here + fraction * before)
        out_ref[0, :, pl.ds(at, LANES)] = total.T
        return carry

    lax.fori_loop(0, columns // LANES, chunk, 0)


def per_device(volume, angle_index, detector_rows, measured):
    layers, row_count, columns = volume.shape
    views = angle_index.shape[0]
    n = lax.axis_size("gz")
    total_depth = layers * n
    own_rows = row_count // n
    each = SUBLANES // own_rows
    groups = views // each
    high_count = n // 8
    height = columns + 2 * (total_depth // 2 + SUBLANES)
    width = columns // COLUMN_PARTS
    count = groups * COLUMN_PARTS
    orders = tuple((part % COLUMN_PARTS) % 2 for part in range(count))
    res_scale = total_depth ** (-0.5)
    view_scale = (views * lax.axis_size("vert")) ** (-0.5)

    smem = pl.BlockSpec(memory_space=pltpu.SMEM)
    vmem = pl.BlockSpec(memory_space=pltpu.VMEM)
    half = (SUBLANES, width)
    full_shape = (count, 2, 2, 2, high_count) + half
    back_shape = (views, height, row_count)
    others = high_count - 1
    stages = 6 + 2 * others
    residual, back = pl.pallas_call(
        functools.partial(forward_kernel, n, orders, total_depth, res_scale, view_scale),
        out_shape=(
            jax.ShapeDtypeStruct(measured.shape, jnp.float32),
            jax.ShapeDtypeStruct(back_shape, jnp.float32),
        ),
        in_specs=[smem, vmem, vmem, pl.BlockSpec(memory_space=pltpu.HBM)],
        out_specs=(vmem, vmem),
        scratch_shapes=[
            pltpu.VMEM((layers, row_count, columns), jnp.float32),
            pltpu.VMEM((layers, height, row_count), jnp.float32),
            pltpu.VMEM((2, each, n * SUBLANES, row_count), jnp.bfloat16),
            pltpu.VMEM((each, width, row_count), jnp.float32),
            pltpu.VMEM(full_shape, jnp.float32),
            pltpu.VMEM(full_shape, jnp.float32),
            pltpu.VMEM((count, 2, 2, high_count) + half, jnp.float32),
            pltpu.VMEM((count, 2, high_count) + half, jnp.float32),
            pltpu.VMEM((count, high_count) + half, jnp.float32),
            pltpu.VMEM((count, others) + half, jnp.float32),
            pltpu.VMEM((count, 2, high_count) + half, jnp.float32),
            pltpu.VMEM((count, high_count) + half, jnp.float32),
            pltpu.VMEM((count, high_count) + half, jnp.float32),
            pltpu.SemaphoreType.DMA((layers,)),
            pltpu.SemaphoreType.DMA((count, stages)),
            pltpu.SemaphoreType.DMA((count, stages)),
        ],
        compiler_params=pltpu.CompilerParams(
            collective_id=0, has_side_effects=True, vmem_limit_bytes=VMEM_LIMIT
        ),
        name="forward",
    )(angle_index, detector_rows.reshape(1, row_count), measured, volume)

    gradient = pl.pallas_call(
        functools.partial(backproject_kernel, total_depth),
        grid=(layers,),
        out_shape=jax.ShapeDtypeStruct((layers, row_count, columns), jnp.float32),
        in_specs=[smem, vmem],
        out_specs=pl.BlockSpec((1, row_count, columns), lambda i: (i, 0, 0)),
        compiler_params=pltpu.CompilerParams(vmem_limit_bytes=VMEM_LIMIT),
        name="backproject",
    )(angle_index, back)
    gradient = lax.psum_scatter(gradient, "vert", scatter_dimension=1, tiled=True)
    return (residual, gradient)


def solution(mesh):
    in_specs = (P("gz", None, None), P("vert"), P(), P("vert", "gz", None))
    out_specs = (P("vert", "gz", None), P("gz", "vert", None))
    return jax.shard_map(
        per_device, mesh=mesh, in_specs=in_specs, out_specs=out_specs, check_vma=False
    )
```

```python
import functools

import jax
import jax.numpy as jnp
from jax import lax
from jax.experimental import pallas as pl
from jax.experimental.pallas import tpu as pltpu
from jax.sharding import PartitionSpec as P

ANGLES = 512
LANES = 128
SUBLANES = 8
COLUMN_PARTS = 4
STAGGER = 0.4
VMEM_LIMIT = 36 * 2**20
FORWARD_LIMIT = 58 * 2**20
CHUNK = 64
MESH = pl.DeviceIdType.MESH


def log2(value):
    return value.bit_length() - 1


def shift_parts(depth, angle):
    product = depth * (2 * angle - ANGLES)
    whole = lax.shift_right_arithmetic(product, jnp.int32(log2(ANGLES)))
    fraction = (product - whole * ANGLES).astype(jnp.float32) * (1.0 / ANGLES)
    return whole, fraction


def ray_weight(angle):
    slope = (2 * angle - ANGLES).astype(jnp.float32) * (1.0 / ANGLES)
    return jnp.sqrt(jnp.full((1, LANES), 1.0 + slope * slope, jnp.float32))


def row_places(det_ref, n, each, own_rows, order):
    row_count = det_ref.shape[1]
    count = n * each * own_rows
    place = lax.broadcasted_iota(jnp.int32, (count, row_count), 0)
    detector = lax.broadcasted_iota(jnp.int32, (count, row_count), 1)
    row = place & (own_rows - 1)
    view = lax.shift_right_logical(place, log2(own_rows)) & (each - 1)
    slot = lax.shift_right_logical(place, log2(own_rows * each))
    high_count = n // 8
    high = slot & (high_count - 1)
    bits = lax.shift_right_logical(slot, log2(high_count))
    second, first, core = bits & 1, lax.shift_right_logical(bits, 1) & 1, lax.shift_right_logical(bits, 2)
    bit1, bit2 = (first, second) if order == 0 else (second, first)
    owner = high * 8 + bit2 * 4 + bit1 * 2 + core
    from_detector = (owner * own_rows + row) == detector
    volume_row = lax.broadcasted_iota(jnp.int32, (row_count, row_count), 0)
    records = (det_ref[...] == volume_row).astype(jnp.float32).astype(jnp.bfloat16)
    places = []
    for i in range(each):
        pick = (from_detector & (view == i)).astype(jnp.float32).astype(jnp.bfloat16)
        moved = lax.dot_general(pick, records, (((1,), (1,)), ((), ())), preferred_element_type=jnp.float32)
        places.append(moved.astype(jnp.bfloat16))
    return places


def two_terms(values):
    high = values.astype(jnp.bfloat16)
    return high, (values - high.astype(jnp.float32)).astype(jnp.bfloat16)


def place_dot(a, b, dims):
    return lax.dot_general(a, b, (dims, ((), ())), preferred_element_type=jnp.float32)


def forward_kernel(n, orders, total_depth, scale, view_scale, angle_ref, det_ref, meas_ref, vol_ref,
                   res_ref, back_ref, slabs, planes, places, partial, own, full,
                   got0, got1, got2, got3, put1, put2, put3, load_sem, send_sem, recv_sem):
    layers, height, row_count = planes.shape
    views, own_rows, columns = meas_ref.shape
    margin = (height - columns) // 2
    each = SUBLANES // own_rows
    count, width = own.shape[0], own.shape[-1]

    me = lax.axis_index("gz")
    high_count = n // 8
    core, bit1, bit2, high = me % 2, (me // 2) % 2, (me // 4) % 2, me // 8
    other_core = me + 1 - 2 * core
    other1, other2 = me + 2 - 4 * bit1, me + 4 - 8 * bit2
    others = [me + 8 * (lax.rem(high + j, high_count) - high) for j in range(1, high_count)]
    base = me * layers - total_depth // 2

    groups = views // each
    slab_count = count // groups
    reach = -(-(total_depth // 2 + 1) // width)
    loads = [
        pltpu.make_async_copy(
            vol_ref.at[:, :, slab * width : (slab + 1) * width], slabs.at[slab], load_sem.at[slab]
        )
        for slab in range(slab_count)
    ]
    for load in loads:
        load.start()
    barrier = pltpu.get_barrier_semaphore()
    for peer in [other_core, other1, other2] + others:
        pl.semaphore_signal(barrier, inc=1, device_id={"gz": peer}, device_id_type=MESH)

    blank = jnp.zeros((margin, row_count), jnp.float32)
    for layer in range(layers):
        planes[layer, :margin, :] = blank
        planes[layer, margin + columns :, :] = blank
    for view in range(views):
        back_ref[view, :margin, :] = blank
        back_ref[view, margin + columns :, :] = blank
    for order in range(2):
        for i, place in enumerate(row_places(det_ref, n, each, own_rows, order)):
            places[order, i] = place
    turned = []

    def turn(slab):
        loads[slab].wait()

        def one(layer, carry):
            for column in range(0, width, LANES):
                at = margin + slab * width + column
                planes[layer, at : at + LANES, :] = slabs[slab, layer, :, column : column + LANES].T
            return carry

        lax.fori_loop(0, layers, one, 0, unroll=2)
        turned.append(slab)

    started = {}
    gather = 3 + len(others)
    last = gather + len(others)

    def start(part, stage, source, target, peer):
        copy = pltpu.make_async_remote_copy(
            src_ref=source, dst_ref=target,
            send_sem=send_sem.at[part, stage], recv_sem=recv_sem.at[part, stage],
            device_id={"gz": peer}, device_id_type=MESH,
        )
        copy.start()
        started[part, stage] = copy

    def arrived(part, stage):
        started[part, stage].wait_recv()

    def project(part):
        group, left = part % groups, (part // groups) * width
        moved = 0.0
        for i in range(each):
            angle = angle_ref[group * each + i]
            steps = [shift_parts(base + layer, angle) for layer in range(layers)]
            weight = ray_weight(angle)

            def chunk(index, carry):
                at = pl.multiple_of(index * CHUNK, CHUNK)
                total = jnp.zeros((CHUNK, row_count), jnp.float32)
                for layer, (whole, fraction) in enumerate(steps):
                    first = margin + left + at + whole
                    here = planes[layer, pl.ds(first, CHUNK), :]
                    following = planes[layer, pl.ds(first + 1, CHUNK), :]
                    total = total + ((1.0 - fraction) * here + fraction * following)
                partial[i, pl.ds(at, CHUNK), :] = total * weight
                return carry

            lax.fori_loop(0, width // CHUNK, chunk, 0)
            for term in two_terms(partial[i]):
                moved = moved + place_dot(places[orders[part], i], term, ((1,), (1,)))
        own[part] = moved.reshape(own.shape[1:])

    def place(part):
        group, left = part % groups, (part // groups) * width
        terms = two_terms(full[part].reshape(-1, width).T)
        for i in range(each):
            view = group * each + i
            matrix = places[orders[part], i]
            moved = place_dot(terms[0], matrix, ((1,), (0,))) + place_dot(terms[1], matrix, ((1,), (0,)))
            back_ref[view, margin + left : margin + left + width, :] = moved * (
                ray_weight(angle_ref[view]) * view_scale
            )

    def event(part, stage):
        if orders[part] == 0:
            a, b, peer_a, peer_b = bit1, bit2, other1, other2
        else:
            a, b, peer_a, peer_b = bit2, bit1, other2, other1
        if stage == 0:
            while len(turned) < min(slab_count, part // groups + reach + 1):
                turn(len(turned))
            project(part)
            if part == 0:
                pl.semaphore_wait(barrier, 3 + len(others))
            start(part, 0, own.at[part, 1 - core], got0.at[part], other_core)
        elif stage == 1:
            arrived(part, 0)
            put1[part] = own[part, core, 1 - a] + got0[part, 1 - a]
            start(part, 1, put1.at[part], got1.at[part], peer_a)
        elif stage == 2:
            arrived(part, 1)
            put2[part] = own[part, core, a, 1 - b] + got0[part, a, 1 - b] + got1[part, 1 - b]
            start(part, 2, put2.at[part], got2.at[part], peer_b)
        elif stage == 3:
            arrived(part, 2)
            put3[part] = own[part, core, a, b] + got0[part, a, b] + got1[part, b] + got2[part]
            for j, peer in enumerate(others):
                start(part, 3 + j, put3.at[part, lax.rem(high + j + 1, high_count)], got3.at[part, j], peer)
        elif stage == 4:
            total = put3[part, high]
            for j in range(len(others)):
                arrived(part, 3 + j)
                total = total + got3[part, j]
            group, column = part % groups, (part // groups) * width
            wanted = [meas_ref[group * each + i, :, column : column + width] for i in range(each)]
            residual = (total - jnp.concatenate(wanted, axis=0)) * scale
            full[part, core, a, b, high] = residual
            mine = full.at[part, core, a, b, high]
            for j, peer in enumerate(others):
                start(part, gather + j, mine, mine, peer)
            for i in range(each):
                res_ref[group * each + i, :, column : column + width] = residual[i * own_rows : (i + 1) * own_rows]
        elif stage == 5:
            for j in range(len(others)):
                arrived(part, gather + j)
            mine = full.at[part, core, a, b]
            start(part, last, mine, mine, peer_b)
        elif stage == 6:
            arrived(part, last)
            mine = full.at[part, core, a]
            start(part, last + 1, mine, mine, peer_a)
        elif stage == 7:
            arrived(part, last + 1)
            mine = full.at[part, core]
            start(part, last + 2, mine, mine, other_core)
        else:
            arrived(part, last + 2)
            place(part)

    for stage, part in sorted(
        ((stage, part) for stage in range(9) for part in range(count)),
        key=lambda item: (item[0] + STAGGER * item[1], -item[0]),
    ):
        event(part, stage)
    for copy in started.values():
        copy.wait_send()


def backproject_kernel(total_depth, angle_ref, back_ref, out_ref):
    views, height, row_count = back_ref.shape
    columns = out_ref.shape[2]
    layers = pl.num_programs(0)
    margin = (height - columns) // 2
    depth = lax.axis_index("gz") * layers - total_depth // 2 + pl.program_id(0)
    steps = [shift_parts(depth, angle_ref[view]) for view in range(views)]

    def chunk(index, carry):
        at = pl.multiple_of(index * LANES, LANES)
        total = jnp.zeros((LANES, row_count), jnp.float32)
        for view, (whole, fraction) in enumerate(steps):
            here = back_ref[view, pl.ds(margin + at - whole, LANES), :]
            before = back_ref[view, pl.ds(margin + at - whole - 1, LANES), :]
            total = total + ((1.0 - fraction) * here + fraction * before)
        out_ref[0, :, pl.ds(at, LANES)] = total.T
        return carry

    lax.fori_loop(0, columns // LANES, chunk, 0, unroll=True)


def per_device(volume, angle_index, detector_rows, measured):
    layers, row_count, columns = volume.shape
    views = angle_index.shape[0]
    n = lax.axis_size("gz")
    total_depth = layers * n
    own_rows = row_count // n
    each = SUBLANES // own_rows
    groups = views // each
    high_count = n // 8
    height = columns + 2 * (total_depth // 2 + SUBLANES)
    width = columns // COLUMN_PARTS
    count = groups * COLUMN_PARTS
    orders = tuple(part % 2 for part in range(count))
    res_scale = total_depth ** (-0.5)
    view_scale = (views * lax.axis_size("vert")) ** (-0.5)

    smem = pl.BlockSpec(memory_space=pltpu.SMEM)
    vmem = pl.BlockSpec(memory_space=pltpu.VMEM)
    half = (SUBLANES, width)
    full_shape = (count, 2, 2, 2, high_count) + half
    back_shape = (views, height, row_count)
    others = high_count - 1
    stages = 6 + 2 * others
    residual, back = pl.pallas_call(
        functools.partial(forward_kernel, n, orders, total_depth, res_scale, view_scale),
        out_shape=(
            jax.ShapeDtypeStruct(measured.shape, jnp.float32),
            jax.ShapeDtypeStruct(back_shape, jnp.float32),
        ),
        in_specs=[smem, vmem, vmem, pl.BlockSpec(memory_space=pltpu.HBM)],
        out_specs=(vmem, vmem),
        scratch_shapes=[
            pltpu.VMEM((COLUMN_PARTS, layers, row_count, width), jnp.float32),
            pltpu.VMEM((layers, height, row_count), jnp.float32),
            pltpu.VMEM((2, each, n * SUBLANES, row_count), jnp.bfloat16),
            pltpu.VMEM((each, width, row_count), jnp.float32),
            pltpu.VMEM(full_shape, jnp.float32),
            pltpu.VMEM(full_shape, jnp.float32),
            pltpu.VMEM((count, 2, 2, high_count) + half, jnp.float32),
            pltpu.VMEM((count, 2, high_count) + half, jnp.float32),
            pltpu.VMEM((count, high_count) + half, jnp.float32),
            pltpu.VMEM((count, others) + half, jnp.float32),
            pltpu.VMEM((count, 2, high_count) + half, jnp.float32),
            pltpu.VMEM((count, high_count) + half, jnp.float32),
            pltpu.VMEM((count, high_count) + half, jnp.float32),
            pltpu.SemaphoreType.DMA((COLUMN_PARTS,)),
            pltpu.SemaphoreType.DMA((count, stages)),
            pltpu.SemaphoreType.DMA((count, stages)),
        ],
        compiler_params=pltpu.CompilerParams(
            collective_id=0, has_side_effects=True, vmem_limit_bytes=FORWARD_LIMIT
        ),
        name="forward",
    )(angle_index, detector_rows.reshape(1, row_count), measured, volume)

    gradient = pl.pallas_call(
        functools.partial(backproject_kernel, total_depth),
        grid=(layers,),
        out_shape=jax.ShapeDtypeStruct((layers, row_count, columns), jnp.float32),
        in_specs=[smem, vmem],
        out_specs=pl.BlockSpec((1, row_count, columns), lambda i: (i, 0, 0)),
        compiler_params=pltpu.CompilerParams(vmem_limit_bytes=VMEM_LIMIT),
        name="backproject",
    )(angle_index, back)
    gradient = lax.psum_scatter(gradient, "vert", scatter_dimension=1, tiled=True)
    return (residual, gradient)


def solution(mesh):
    in_specs = (P("gz", None, None), P("vert"), P(), P("vert", "gz", None))
    out_specs = (P("vert", "gz", None), P("gz", "vert", None))
    return jax.shard_map(
        per_device, mesh=mesh, in_specs=in_specs, out_specs=out_specs, check_vma=False
    )
```

```python
import functools

import jax
import jax.numpy as jnp
from jax import lax
from jax.experimental import pallas as pl
from jax.experimental.pallas import tpu as pltpu
from jax.sharding import PartitionSpec as P

ANGLES = 512
LANES = 128
SUBLANES = 8
COLUMN_PARTS = 4
STAGGER = 0.35
VMEM_LIMIT = 36 * 2**20
FORWARD_LIMIT = 50 * 2**20
CHUNK = 64
MESH = pl.DeviceIdType.MESH


def log2(value):
    return value.bit_length() - 1


def shift_parts(depth, angle):
    product = depth * (2 * angle - ANGLES)
    whole = lax.shift_right_arithmetic(product, jnp.int32(log2(ANGLES)))
    fraction = (product - whole * ANGLES).astype(jnp.float32) * (1.0 / ANGLES)
    return whole, fraction


def ray_weight(angle):
    slope = (2 * angle - ANGLES).astype(jnp.float32) * (1.0 / ANGLES)
    return jnp.sqrt(jnp.full((1, LANES), 1.0 + slope * slope, jnp.float32))


def row_places(det_ref, n, each, own_rows, order):
    row_count = det_ref.shape[1]
    count = n * each * own_rows
    place = lax.broadcasted_iota(jnp.int32, (count, row_count), 0)
    detector = lax.broadcasted_iota(jnp.int32, (count, row_count), 1)
    row = place & (own_rows - 1)
    view = lax.shift_right_logical(place, log2(own_rows)) & (each - 1)
    slot = lax.shift_right_logical(place, log2(own_rows * each))
    high_count = n // 8
    high = slot & (high_count - 1)
    bits = lax.shift_right_logical(slot, log2(high_count))
    second, first, core = bits & 1, lax.shift_right_logical(bits, 1) & 1, lax.shift_right_logical(bits, 2)
    bit1, bit2 = (first, second) if order == 0 else (second, first)
    owner = high * 8 + bit2 * 4 + bit1 * 2 + core
    from_detector = (owner * own_rows + row) == detector
    volume_row = lax.broadcasted_iota(jnp.int32, (row_count, row_count), 0)
    records = (det_ref[...] == volume_row).astype(jnp.float32).astype(jnp.bfloat16)
    places = []
    for i in range(each):
        pick = (from_detector & (view == i)).astype(jnp.float32).astype(jnp.bfloat16)
        moved = lax.dot_general(pick, records, (((1,), (1,)), ((), ())), preferred_element_type=jnp.float32)
        places.append(moved.astype(jnp.bfloat16))
    return places


def two_terms(values):
    high = values.astype(jnp.bfloat16)
    return high, (values - high.astype(jnp.float32)).astype(jnp.bfloat16)


def place_dot(a, b, dims):
    return lax.dot_general(a, b, (dims, ((), ())), preferred_element_type=jnp.float32)


def forward_kernel(n, orders, total_depth, scale, view_scale, angle_ref, det_ref, meas_ref, vol_ref,
                   res_ref, back_ref, slabs, planes, places, partial, own, full,
                   got0, got1, got2, got3, put1, put2, put3, load_sem, send_sem, recv_sem):
    layers, height, row_count = planes.shape
    views, own_rows, columns = meas_ref.shape
    margin = (height - columns) // 2
    each = SUBLANES // own_rows
    count, width = own.shape[0], own.shape[-1]

    me = lax.axis_index("gz")
    high_count = n // 8
    core, bit1, bit2, high = me % 2, (me // 2) % 2, (me // 4) % 2, me // 8
    other_core = me + 1 - 2 * core
    other1, other2 = me + 2 - 4 * bit1, me + 4 - 8 * bit2
    others = [me + 8 * (lax.rem(high + j, high_count) - high) for j in range(1, high_count)]
    base = me * layers - total_depth // 2

    groups = views // each
    slab_count = count // groups
    reach = -(-(total_depth // 2 + 1) // width)
    loads = [
        pltpu.make_async_copy(
            vol_ref.at[:, :, slab * width : (slab + 1) * width], slabs.at[slab], load_sem.at[slab]
        )
        for slab in range(slab_count)
    ]
    for load in loads:
        load.start()
    barrier = pltpu.get_barrier_semaphore()
    for peer in [other_core, other1, other2] + others:
        pl.semaphore_signal(barrier, inc=1, device_id={"gz": peer}, device_id_type=MESH)

    blank = jnp.zeros((margin, row_count), jnp.float32)
    for layer in range(layers):
        planes[layer, :margin, :] = blank
        planes[layer, margin + columns :, :] = blank
    for view in range(views):
        back_ref[view, :margin, :] = blank
        back_ref[view, margin + columns :, :] = blank
    for order in range(2):
        for i, place in enumerate(row_places(det_ref, n, each, own_rows, order)):
            places[order, i] = place
    turned = []

    def turn(slab):
        loads[slab].wait()

        def one(layer, carry):
            for column in range(0, width, LANES):
                at = margin + slab * width + column
                planes[layer, at : at + LANES, :] = slabs[slab, layer, :, column : column + LANES].T
            return carry

        lax.fori_loop(0, layers, one, 0, unroll=2)
        turned.append(slab)

    started = {}
    gather = 3 + len(others)
    last = gather + len(others)

    def start(part, stage, source, target, peer):
        copy = pltpu.make_async_remote_copy(
            src_ref=source, dst_ref=target,
            send_sem=send_sem.at[part, stage], recv_sem=recv_sem.at[part, stage],
            device_id={"gz": peer}, device_id_type=MESH,
        )
        copy.start()
        started[part, stage] = copy

    def arrived(part, stage):
        started[part, stage].wait_recv()

    def project(part):
        group, left = part % groups, (part // groups) * width
        moved = 0.0
        for i in range(each):
            angle = angle_ref[group * each + i]
            steps = [shift_parts(base + layer, angle) for layer in range(layers)]
            weight = ray_weight(angle)

            def chunk(index, carry):
                at = pl.multiple_of(index * CHUNK, CHUNK)
                total = jnp.zeros((CHUNK, row_count), jnp.float32)
                for layer, (whole, fraction) in enumerate(steps):
                    first = margin + left + at + whole
                    here = planes[layer, pl.ds(first, CHUNK), :]
                    following = planes[layer, pl.ds(first + 1, CHUNK), :]
                    total = total + ((1.0 - fraction) * here + fraction * following)
                partial[i, pl.ds(at, CHUNK), :] = total * weight
                return carry

            lax.fori_loop(0, width // CHUNK, chunk, 0)
            for term in two_terms(partial[i]):
                moved = moved + place_dot(places[orders[part], i], term, ((1,), (1,)))
        own[part] = moved.reshape(own.shape[1:])

    def place(part):
        group, left = part % groups, (part // groups) * width
        terms = two_terms(full[part].reshape(-1, width).T)
        for i in range(each):
            view = group * each + i
            matrix = places[orders[part], i]
            moved = place_dot(terms[0], matrix, ((1,), (0,))) + place_dot(terms[1], matrix, ((1,), (0,)))
            back_ref[view, margin + left : margin + left + width, :] = moved * (
                ray_weight(angle_ref[view]) * view_scale
            )

    def event(part, stage):
        if orders[part] == 0:
            a, b, peer_a, peer_b = bit1, bit2, other1, other2
        else:
            a, b, peer_a, peer_b = bit2, bit1, other2, other1
        if stage == 0:
            while len(turned) < min(slab_count, part // groups + reach + 1):
                turn(len(turned))
            project(part)
            if part == 0:
                pl.semaphore_wait(barrier, 3 + len(others))
            start(part, 0, own.at[part, 1 - core], got0.at[part], other_core)
        elif stage == 1:
            arrived(part, 0)
            put1[part] = own[part, core, 1 - a] + got0[part, 1 - a]
            start(part, 1, put1.at[part], got1.at[part], peer_a)
        elif stage == 2:
            arrived(part, 1)
            put2[part] = own[part, core, a, 1 - b] + got0[part, a, 1 - b] + got1[part, 1 - b]
            start(part, 2, put2.at[part], got2.at[part], peer_b)
        elif stage == 3:
            arrived(part, 2)
            put3[part] = own[part, core, a, b] + got0[part, a, b] + got1[part, b] + got2[part]
            for j, peer in enumerate(others):
                start(part, 3 + j, put3.at[part, lax.rem(high + j + 1, high_count)], got3.at[part, j], peer)
        elif stage == 4:
            total = put3[part, high]
            for j in range(len(others)):
                arrived(part, 3 + j)
                total = total + got3[part, j]
            group, column = part % groups, (part // groups) * width
            wanted = [meas_ref[group * each + i, :, column : column + width] for i in range(each)]
            residual = (total - jnp.concatenate(wanted, axis=0)) * scale
            full[part, core, a, b, high] = residual
            mine = full.at[part, core, a, b, high]
            for j, peer in enumerate(others):
                start(part, gather + j, mine, mine, peer)
            for i in range(each):
                res_ref[group * each + i, :, column : column + width] = residual[i * own_rows : (i + 1) * own_rows]
        elif stage == 5:
            for j in range(len(others)):
                arrived(part, gather + j)
            mine = full.at[part, core, a, b]
            start(part, last, mine, mine, peer_b)
        elif stage == 6:
            arrived(part, last)
            mine = full.at[part, core, a]
            start(part, last + 1, mine, mine, peer_a)
        elif stage == 7:
            arrived(part, last + 1)
            mine = full.at[part, core]
            start(part, last + 2, mine, mine, other_core)
        else:
            arrived(part, last + 2)
            place(part)

    for stage, part in sorted(
        ((stage, part) for stage in range(9) for part in range(count)),
        key=lambda item: (item[0] + STAGGER * item[1], -item[0]),
    ):
        event(part, stage)
    for copy in started.values():
        copy.wait_send()


def backproject_kernel(total_depth, angle_ref, back_ref, out_ref):
    views, height, row_count = back_ref.shape
    columns = out_ref.shape[2]
    layers = pl.num_programs(0)
    margin = (height - columns) // 2
    depth = lax.axis_index("gz") * layers - total_depth // 2 + pl.program_id(0)
    steps = [shift_parts(depth, angle_ref[view]) for view in range(views)]

    def chunk(index, carry):
        at = pl.multiple_of(index * LANES, LANES)
        total = jnp.zeros((LANES, row_count), jnp.float32)
        for view, (whole, fraction) in enumerate(steps):
            here = back_ref[view, pl.ds(margin + at - whole, LANES), :]
            before = back_ref[view, pl.ds(margin + at - whole - 1, LANES), :]
            total = total + ((1.0 - fraction) * here + fraction * before)
        out_ref[0, :, pl.ds(at, LANES)] = total.T
        return carry

    lax.fori_loop(0, columns // LANES, chunk, 0, unroll=True)


def per_device(volume, angle_index, detector_rows, measured):
    layers, row_count, columns = volume.shape
    views = angle_index.shape[0]
    n = lax.axis_size("gz")
    total_depth = layers * n
    own_rows = row_count // n
    each = SUBLANES // own_rows
    groups = views // each
    high_count = n // 8
    height = columns + 2 * (total_depth // 2 + SUBLANES)
    width = columns // COLUMN_PARTS
    count = groups * COLUMN_PARTS
    orders = tuple(part % 2 for part in range(count))
    res_scale = total_depth ** (-0.5)
    view_scale = (views * lax.axis_size("vert")) ** (-0.5)

    smem = pl.BlockSpec(memory_space=pltpu.SMEM)
    vmem = pl.BlockSpec(memory_space=pltpu.VMEM)
    half = (SUBLANES, width)
    full_shape = (count, 2, 2, 2, high_count) + half
    back_shape = (views, height, row_count)
    others = high_count - 1
    stages = 6 + 2 * others
    residual, back = pl.pallas_call(
        functools.partial(forward_kernel, n, orders, total_depth, res_scale, view_scale),
        out_shape=(
            jax.ShapeDtypeStruct(measured.shape, jnp.float32),
            jax.ShapeDtypeStruct(back_shape, jnp.float32),
        ),
        in_specs=[smem, vmem, vmem, pl.BlockSpec(memory_space=pltpu.HBM)],
        out_specs=(vmem, vmem),
        scratch_shapes=[
            pltpu.VMEM((COLUMN_PARTS, layers, row_count, width), jnp.float32),
            pltpu.VMEM((layers, height, row_count), jnp.float32),
            pltpu.VMEM((2, each, n * SUBLANES, row_count), jnp.bfloat16),
            pltpu.VMEM((each, width, row_count), jnp.float32),
            pltpu.VMEM(full_shape, jnp.float32),
            pltpu.VMEM(full_shape, jnp.float32),
            pltpu.VMEM((count, 2, 2, high_count) + half, jnp.float32),
            pltpu.VMEM((count, 2, high_count) + half, jnp.float32),
            pltpu.VMEM((count, high_count) + half, jnp.float32),
            pltpu.VMEM((count, others) + half, jnp.float32),
            pltpu.VMEM((count, 2, high_count) + half, jnp.float32),
            pltpu.VMEM((count, high_count) + half, jnp.float32),
            pltpu.VMEM((count, high_count) + half, jnp.float32),
            pltpu.SemaphoreType.DMA((COLUMN_PARTS,)),
            pltpu.SemaphoreType.DMA((count, stages)),
            pltpu.SemaphoreType.DMA((count, stages)),
        ],
        compiler_params=pltpu.CompilerParams(
            collective_id=0, has_side_effects=True, vmem_limit_bytes=FORWARD_LIMIT
        ),
        name="forward",
    )(angle_index, detector_rows.reshape(1, row_count), measured, volume)

    gradient = pl.pallas_call(
        functools.partial(backproject_kernel, total_depth),
        grid=(layers,),
        out_shape=jax.ShapeDtypeStruct((layers, row_count, columns), jnp.float32),
        in_specs=[smem, vmem],
        out_specs=pl.BlockSpec((1, row_count, columns), lambda i: (i, 0, 0)),
        compiler_params=pltpu.CompilerParams(vmem_limit_bytes=VMEM_LIMIT),
        name="backproject",
    )(angle_index, back)
    gradient = lax.psum_scatter(gradient, "vert", scatter_dimension=1, tiled=True)
    return (residual, gradient)


def solution(mesh):
    in_specs = (P("gz", None, None), P("vert"), P(), P("vert", "gz", None))
    out_specs = (P("vert", "gz", None), P("gz", "vert", None))
    return jax.shard_map(
        per_device, mesh=mesh, in_specs=in_specs, out_specs=out_specs, check_vma=False
    )
```
